256 devices in a mesh: grp: 4 (over z_hi), freq: 64 (over z_lo, y, x, core).
Axes of the slice: x: 4, y: 4, z: 8 (z_hi: 4, z_lo: 2; z = z_hi * 2 + z_lo), core: 2. Of those that a mesh axis runs over, the one named last changes fastest.
Arguments:
- sources: bfloat16 [1024, 262144], P('freq', 'grp'), may hold values from -6 to 6
- panel_pos: float32 [3, 262144], P(None, 'grp'), may hold values from -1 to 1
- panel_blade: int32 [262144], P('grp'), may hold values from 0 to 3
- observer_table: float32 [3, 2048], replicated, may hold values from -8 to 8, as said below
- observer_index: int32 [32], replicated, may hold values from 0 to 2047
Outputs:
- spectra: float32 [512, 4, 2, 32], P('freq', 'grp')
The draws below stay inside these ranges and needn't reach their ends.
Inputs may be any that keep to these rules, and one draw needn't show every extreme that they name: `observer_table`: each observer lies 3 to 8 units from the anchor (0, 0, 0).
All inputs are finite; a program needn't handle non-finite values.
Results may differ from the reference program's by a relative error of at most 0.0047.
Values may be sent and summed in bfloat16 or wider, within the bound.
A program may use at most 64 MiB of HBM per device.

```python
import math
import jax
import jax.numpy as jnp
from jax import lax

NT = 1024
NF = 512
NCOMP = 4
NOBS = 32
NOBS_ALL = 2048
PANELS = 262144


def draw_observer_table(key, part):
    key_height = jax.random.fold_in(key, 11)
    key_turn = jax.random.fold_in(key, 12)
    key_radius = jax.random.fold_in(key, 13)
    height = jax.random.uniform(key_height, (NOBS_ALL,), jnp.float32, -1.0, 1.0)
    turn_angle = jax.random.uniform(key_turn, (NOBS_ALL,), jnp.float32, -math.pi, math.pi)
    uniform_part = jax.random.uniform(key_radius, (NOBS_ALL,), jnp.float32, 0.0, 1.0)
    radius = 3.0 + 5.0 * uniform_part
    cycle_radius = jnp.sqrt(jnp.maximum(1.0 - height * height, 0.0))
    return jnp.stack([radius * cycle_radius * jnp.cos(turn_angle), radius * cycle_radius * jnp.sin(turn_angle), radius * height]).astype(jnp.float32)


def place_ends(result, own_key, least, largest):
    spot = [jax.random.randint(jax.random.fold_in(own_key, axis), (), 0, length) for axis, length in enumerate(result.shape)]
    widest = result.shape.index(max(result.shape))
    beside = spot[:widest] + [(spot[widest] + 1) % result.shape[widest]] + spot[widest + 1:]
    return result.at[tuple(spot)].set(least).at[tuple(beside)].set(largest)


def level_of(rng, dims, shards, low, largest):
    gain = 1.0
    for position, blocks in shards:
        draws = jax.random.uniform(jax.random.fold_in(jax.random.fold_in(rng, 6), position), (blocks,), jnp.float32, low / len(shards), largest / len(shards))
        gain = gain * jnp.repeat(jnp.exp(draws), dims[position] // blocks).reshape((-1,) + (1,) * (len(dims) - 1 - position))
    return gain


def normal_values(own_key, shape, deviation, limit, split=(), kind=jnp.bfloat16):
    drawn = deviation * jax.random.normal(own_key, shape, jnp.float32)
    if split:
        drawn = drawn * level_of(own_key, shape, split, -0.22, 0.18)
    return jnp.clip(drawn, -limit, limit).astype(kind)


def setup_inputs(seed: int = 0) -> dict:
    arg_keys = jax.random.split(jax.random.key(seed), 6)
    return {
        "sources": normal_values(arg_keys[0], (NT, PANELS), 1.0, 6.0, ((0, 64), (1, 4))),
        "panel_pos": jnp.clip(jax.random.uniform(arg_keys[1], (3, PANELS), jnp.float32, -1.0, 1.0) * level_of(arg_keys[1], (3, PANELS), ((1, 4),), -0.4, 0.0), -1.0, 1.0),
        "panel_blade": place_ends(jax.random.randint(arg_keys[2], (PANELS,), 0, NCOMP), jax.random.fold_in(arg_keys[2], 1), 0, NCOMP - 1).astype(jnp.int32),
        "observer_table": draw_observer_table(jax.random.fold_in(arg_keys[5], 71), 0),
        "observer_index": place_ends(jax.random.randint(arg_keys[4], (NOBS,), 0, NOBS_ALL), jax.random.fold_in(arg_keys[4], 1), 0, NOBS_ALL - 1).astype(jnp.int32),
    }


wave_step = 0.04

def transform_table():
    row_index = jnp.arange(2 * NF, dtype=jnp.int32)
    samples = jnp.arange(NT, dtype=jnp.int32)
    frequency = row_index // 2
    parity = row_index % 2
    turn_count = frequency[:, None] * samples[None, :] % NT
    angle_table = 2.0 * math.pi / NT * turn_count.astype(jnp.float32)
    values = jnp.where(parity[:, None] == 0, jnp.cos(angle_table), -jnp.sin(angle_table))
    return (values / math.sqrt(NT)).astype(jnp.bfloat16)

def distances(positions, observers):
    offset_x = observers[0][:, None] - positions[0][None, :]
    offset_y = observers[1][:, None] - positions[1][None, :]
    offset_z = observers[2][:, None] - positions[2][None, :]
    return jnp.sqrt(offset_x * offset_x + offset_y * offset_y + offset_z * offset_z)

def blade_masks(blades):
    return (blades[None, :] == jnp.arange(NCOMP, dtype=jnp.int32)[:, None]).astype(jnp.bfloat16)

def frequency_term(frequency, spectrum_pair, blade_mask, distance, amplitude):
    wavenumber = wave_step * frequency.astype(jnp.float32)
    phase_angle = wavenumber * distance
    green_matrix = jnp.concatenate([jnp.cos(phase_angle) * amplitude, -jnp.sin(phase_angle) * amplitude], axis=0).astype(jnp.bfloat16)
    weighted = jnp.concatenate([spectrum_pair[0][None, :] * blade_mask, spectrum_pair[1][None, :] * blade_mask], axis=0)
    product = lax.dot_general(weighted, green_matrix, (((1,), (1,)), ((), ())), preferred_element_type=jnp.float32)
    blade_count = blade_mask.shape[0]
    observer_count = distance.shape[0]
    real_part = product[:blade_count, :observer_count] - product[blade_count:, observer_count:]
    imag_part = product[:blade_count, observer_count:] + product[blade_count:, :observer_count]
    return jnp.stack([real_part, imag_part], axis=1)

def reference(sources, panel_pos, panel_blade, observer_table, observer_index):
    observers = observer_table[:, observer_index]
    spectrum = jnp.dot(transform_table(), sources, preferred_element_type=jnp.float32).astype(jnp.bfloat16)
    spectrum = spectrum.reshape(NF, 2, spectrum.shape[1])
    distance = distances(panel_pos, observers)
    amplitude = 0.25 / (math.pi * distance)
    blade_mask = blade_masks(panel_blade)

    def per_frequency(element):
        return frequency_term(element[0], element[1], blade_mask, distance, amplitude)
    return lax.map(per_frequency, (jnp.arange(NF, dtype=jnp.int32), spectrum))
```

```python
import functools
import math

import jax
import jax.numpy as jnp
from jax import lax
from jax.experimental import pallas as pl
from jax.experimental.pallas import tpu as pltpu
from jax.sharding import PartitionSpec as P

NT = 1024
NF = 512
NCOMP = 4
NOBS = 32

wave_step = 0.04

FREQ_RANKS = 64
GRP_RANKS = 4
ROWS = NT // FREQ_RANKS
CHUNKS = 4
WIDTH = 256
SHARE = CHUNKS * WIDTH
JOINT = 4
TILES = NF // JOINT
UNROLL = 16
STEPS = TILES // UNROLL
MESH = pl.DeviceIdType.MESH


def transform_table():
    row_index = jnp.arange(2 * NF, dtype=jnp.int32)
    samples = jnp.arange(NT, dtype=jnp.int32)
    frequency = row_index // 8 * JOINT + row_index % JOINT
    parity = row_index // JOINT % 2
    turn_count = frequency[:, None] * samples[None, :] % NT
    angle_table = 2.0 * math.pi / NT * turn_count.astype(jnp.float32)
    values = jnp.where(parity[:, None] == 0, jnp.cos(angle_table), -jnp.sin(angle_table))
    return (values / math.sqrt(NT)).astype(jnp.bfloat16)


def partner(me, i):
    e = i * 37 % FREQ_RANKS
    core = (me + e) % 2
    x = (me // 2 + e // 2) % 4
    y = (me // 8 + e // 8) % 4
    z = (me // 32 + e // 32) % 2
    return z * 32 + y * 8 + x * 2 + core


def kernel(
    source_hbm, table_hbm, panel_ref, observer_ref, out_ref,
    source, table, received, state, green, weighted, total, partial, gathered, share_out, share_in,
    load_sem, table_sem, send_sem, recv_sem, sum_send, sum_recv, share_send, share_recv,
):
    me = lax.axis_index("freq")
    group = lax.axis_index("grp")
    load = pltpu.make_async_copy(source_hbm, source, load_sem)
    load.start()
    table_load = pltpu.make_async_copy(table_hbm, table, table_sem)
    table_load.start()

    barrier = pltpu.get_barrier_semaphore()

    def greet(i, carry):
        pl.semaphore_signal(
            barrier, inc=1, device_id={"freq": partner(me, i)}, device_id_type=MESH
        )
        return carry

    lax.fori_loop(1, FREQ_RANKS, greet, 0)
    for i in range(1, GRP_RANKS):
        pl.semaphore_signal(
            barrier, inc=1, device_id={"grp": (group + i) % GRP_RANKS}, device_id_type=MESH
        )
    load.wait()
    pl.semaphore_wait(barrier, FREQ_RANKS - 1 + GRP_RANKS - 1)

    own_rows = pl.ds(pl.multiple_of(me * ROWS, ROWS), ROWS)

    def columns(device, chunk):
        return pl.ds(pl.multiple_of(device * SHARE + chunk * WIDTH, WIDTH), WIDTH)

    for chunk in range(CHUNKS):

        def send(i, carry):
            device = partner(me, i)
            pltpu.make_async_remote_copy(
                src_ref=source.at[:, columns(device, chunk)],
                dst_ref=received.at[chunk, own_rows, :],
                send_sem=send_sem.at[chunk],
                recv_sem=recv_sem.at[chunk],
                device_id={"freq": device},
                device_id_type=MESH,
            ).start()
            return carry

        pltpu.make_async_copy(
            source.at[:, columns(me, chunk)],
            received.at[chunk, own_rows, :],
            recv_sem.at[chunk],
        ).start()
        lax.fori_loop(1, FREQ_RANKS, send, 0)

    def seed(chunk):
        for half in range(WIDTH // 128):
            squares = None
            for axis in range(3):
                row = panel_ref[axis : axis + 1, pl.ds(chunk * WIDTH + half * 128, 128)]
                column = jnp.broadcast_to(row, (128, 128)).T
                offset = observer_ref[axis : axis + 1, :] - column
                squares = offset * offset if squares is None else squares + offset * offset
            inverse = lax.rsqrt(squares)
            distance = squares * inverse
            amplitude = (0.25 / math.pi) * inverse
            angle = wave_step * distance
            w = angle * angle
            cos1 = 1.0 + w * (-1 / 2 + w * (1 / 24 + w * (-1 / 720 + w * (1 / 40320 - w * (1 / 3628800)))))
            sin1 = angle * (1.0 + w * (-1 / 6 + w * (1 / 120 + w * (-1 / 5040 + w * (1 / 362880)))))
            cos2 = cos1 * cos1 - sin1 * sin1
            sin2 = 2.0 * sin1 * cos1
            cos3 = cos2 * cos1 - sin2 * sin1
            sin3 = sin2 * cos1 + cos2 * sin1
            cos4 = cos2 * cos2 - sin2 * sin2
            sin4 = 2.0 * sin2 * cos2
            lane = lax.broadcasted_iota(jnp.int32, (128, 128), 1) // NOBS
            cos_j = jnp.where(lane == 0, 1.0, jnp.where(lane == 1, cos1, jnp.where(lane == 2, cos2, cos3)))
            sin_j = jnp.where(lane == 0, 0.0, jnp.where(lane == 1, sin1, jnp.where(lane == 2, sin2, sin3)))
            rows = pl.ds(half * 128, 128)
            state[0, rows, :] = 2.0 * cos4
            state[1, rows, :] = amplitude * (cos_j * cos4 + sin_j * sin4)
            state[2, rows, :] = amplitude * cos_j
            state[3, rows, :] = -amplitude * (sin_j * cos4 - cos_j * sin4)
            state[4, rows, :] = -amplitude * sin_j

    def grow(slot, step):
        for block in range(WIDTH // 16):
            rows = pl.ds(block * 16, 16)
            twice = state[0, rows, :]
            re_old, re_new = state[1, rows, :], state[2, rows, :]
            im_old, im_new = state[3, rows, :], state[4, rows, :]
            for u in range(UNROLL):
                tile = step * UNROLL + u
                green[slot, tile, rows, 0:128] = re_new.astype(jnp.bfloat16)
                green[slot, tile, rows, 128:256] = im_new.astype(jnp.bfloat16)
                re_old, re_new = re_new, twice * re_new - re_old
                im_old, im_new = im_new, twice * im_new - im_old
            state[1, rows, :] = re_old
            state[2, rows, :] = re_new
            state[3, rows, :] = im_old
            state[4, rows, :] = im_new

    def grow_all(slot):
        lax.fori_loop(0, STEPS, lambda step, c: (grow(slot, step), c)[1], 0)

    seed(0)
    grow_all(0)
    seed(1)
    grow_all(1)
    table_load.wait()

    sublane = lax.broadcasted_iota(jnp.int32, (8, 128), 0)
    lane_joint = lax.broadcasted_iota(jnp.int32, (8, 128), 1) // NOBS
    keep_a = (sublane == lane_joint).astype(jnp.float32)
    keep_c = (sublane == lane_joint + JOINT).astype(jnp.float32)

    def transform(chunk):
        blades = panel_ref[3:4, pl.ds(chunk * WIDTH, WIDTH)]
        masks = [(blades == float(b)).astype(jnp.float32).reshape(1, 1, WIDTH) for b in range(NCOMP)]

        def part(i, carry):
            spectrum = jnp.dot(
                table[pl.ds(pl.multiple_of(i * 256, 256), 256), :],
                received[chunk],
                preferred_element_type=jnp.float32,
            ).reshape(32, 8, WIDTH)
            for pair in range(NCOMP // 2):
                both = jnp.concatenate([spectrum * masks[2 * pair], spectrum * masks[2 * pair + 1]], axis=1)
                weighted[pl.ds(i * 32, 32), pl.ds(16 * pair, 16), :] = both.astype(jnp.bfloat16)
            return carry

        lax.fori_loop(0, 4, part, 0)

    def pressure(value):
        sums = []
        for blade in range(NCOMP):
            re_side = value[8 * blade : 8 * blade + 8, 0:128]
            im_side = value[8 * blade : 8 * blade + 8, 128:256]
            sums.append(jnp.sum(re_side * keep_a - im_side * keep_c, axis=0, keepdims=True))
            sums.append(jnp.sum(im_side * keep_a + re_side * keep_c, axis=0, keepdims=True))
        return jnp.concatenate(sums, axis=0)

    def send_sums(step):
        for u in range(UNROLL // 2):
            device = step * (UNROLL // 2) + u

            @pl.when(device != me)
            def _():
                pltpu.make_async_remote_copy(
                    src_ref=partial.at[device],
                    dst_ref=gathered.at[me],
                    send_sem=sum_send,
                    recv_sem=sum_recv,
                    device_id={"freq": device},
                    device_id_type=MESH,
                ).start()

    for chunk in range(CHUNKS):
        pltpu.make_async_copy(received.at[chunk], received.at[chunk], recv_sem.at[chunk]).wait()
        transform(chunk)
        slot = chunk % 2
        ahead = chunk + 2 < CHUNKS
        last = chunk == CHUNKS - 1
        if ahead:
            seed(chunk + 2)

        def contract(step, carry):
            if last:

                @pl.when(step > 0)
                def _():
                    send_sums(step - 1)

            rows = []
            for u in range(UNROLL):
                tile = step * UNROLL + u
                product = jnp.dot(weighted[tile], green[slot, tile], preferred_element_type=jnp.float32)
                if chunk > 0:
                    product = total[tile] + product
                if last:
                    rows.append(pressure(product))
                else:
                    total[tile] = product
            if last:
                for u in range(UNROLL // 2):
                    both = jnp.concatenate([rows[2 * u], rows[2 * u + 1]], axis=0)
                    partial[step * (UNROLL // 2) + u] = both.astype(jnp.bfloat16)
            if ahead:
                grow(slot, step)
            return carry

        lax.fori_loop(0, STEPS, contract, 0)

    own = pltpu.make_async_copy(partial.at[me], gathered.at[me], sum_recv)
    own.start()
    send_sums(STEPS - 1)
    pltpu.make_async_copy(gathered, gathered, sum_recv).wait()

    def add(i, carry):
        return carry + jnp.sum(gathered[pl.ds(i * 8, 8)].astype(jnp.float32), axis=0)

    summed = lax.fori_loop(0, FREQ_RANKS // 8, add, jnp.zeros((16, 128), jnp.float32))
    for blade in range(NCOMP):
        share_out[blade, 0:2, :] = summed[2 * blade : 2 * blade + 2, :]
        share_out[blade, 2:4, :] = summed[8 + 2 * blade : 8 + 2 * blade + 2, :]
        share_out[blade, 4:8, :] = jnp.zeros((4, 128), jnp.float32)
    for i in range(1, GRP_RANKS):
        other = (group + i) % GRP_RANKS
        pltpu.make_async_remote_copy(
            src_ref=share_out.at[other],
            dst_ref=share_in.at[group],
            send_sem=share_send,
            recv_sem=share_recv,
            device_id={"grp": other},
            device_id_type=MESH,
        ).start()
    pltpu.make_async_copy(share_out.at[group], share_in.at[group], share_recv).start()
    pltpu.make_async_copy(share_in, share_in, share_recv).wait()
    result = share_in[0] + share_in[1] + share_in[2] + share_in[3]
    for m in range(2):
        for j in range(JOINT):
            for part in range(2):
                out_ref[JOINT * m + j, part : part + 1, :] = result[
                    2 * m + part : 2 * m + part + 1, NOBS * j : NOBS * (j + 1)
                ]

    for chunk in range(CHUNKS):
        sent = received.at[chunk, pl.ds(0, ROWS * (FREQ_RANKS - 1)), :]
        pltpu.make_async_copy(sent, sent, send_sem.at[chunk]).wait()
    sent = gathered.at[pl.ds(0, FREQ_RANKS - 1)]
    pltpu.make_async_copy(sent, sent, sum_send).wait()
    sent = share_in.at[pl.ds(0, GRP_RANKS - 1)]
    pltpu.make_async_copy(sent, sent, share_send).wait()


def body(sources, panel_pos, panel_blade, observer_table, observer_index):
    me = lax.axis_index("freq")
    observers = jnp.tile(observer_table[:, observer_index], (1, JOINT))
    observers = jnp.pad(observers, ((0, 5), (0, 0)))
    position = lax.dynamic_slice_in_dim(panel_pos, me * SHARE, SHARE, 1)
    blade = lax.dynamic_slice_in_dim(panel_blade, me * SHARE, SHARE, 0).astype(jnp.float32)
    panels = jnp.concatenate([position, blade[None], jnp.zeros((4, SHARE), jnp.float32)], axis=0)
    bf16, f32 = jnp.bfloat16, jnp.float32
    dma = pltpu.SemaphoreType.DMA
    out = pl.pallas_call(
        kernel,
        out_shape=jax.ShapeDtypeStruct((8, 2, NOBS), f32),
        in_specs=[
            pl.BlockSpec(memory_space=pl.ANY),
            pl.BlockSpec(memory_space=pl.ANY),
            pl.BlockSpec(memory_space=pltpu.VMEM),
            pl.BlockSpec(memory_space=pltpu.VMEM),
        ],
        out_specs=pl.BlockSpec(memory_space=pltpu.VMEM),
        scratch_shapes=[
            pltpu.VMEM((ROWS, FREQ_RANKS * SHARE), bf16),
            pltpu.VMEM((2 * NF, NT), bf16),
            pltpu.VMEM((CHUNKS, NT, WIDTH), bf16),
            pltpu.VMEM((5, WIDTH, 128), f32),
            pltpu.VMEM((2, TILES, WIDTH, 256), bf16),
            pltpu.VMEM((TILES, 32, WIDTH), bf16),
            pltpu.VMEM((TILES, 32, 256), f32),
            pltpu.VMEM((FREQ_RANKS, 16, 128), bf16),
            pltpu.VMEM((FREQ_RANKS, 16, 128), bf16),
            pltpu.VMEM((NCOMP, 8, 128), f32),
            pltpu.VMEM((GRP_RANKS, 8, 128), f32),
            dma, dma, dma((CHUNKS,)), dma((CHUNKS,)), dma, dma, dma, dma,
        ],
        compiler_params=pltpu.CompilerParams(
            collective_id=0, has_side_effects=True, vmem_limit_bytes=60 * 2**20
        ),
    )(sources, transform_table(), panels, observers)
    return out[:, None]


def solution(mesh):
    in_specs = (P("freq", "grp"), P(None, "grp"), P("grp"), P(), P())
    out_specs = P("freq", "grp", None, None)
    return jax.shard_map(body, mesh=mesh, in_specs=in_specs, out_specs=out_specs, check_vma=False)
```

```python
import math

import jax
import jax.numpy as jnp
import numpy as np
from jax import lax
from jax.experimental import pallas as pl
from jax.experimental.pallas import tpu as pltpu
from jax.sharding import PartitionSpec as P

NT = 1024
NF = 512
NCOMP = 4
NOBS = 32

wave_step = 0.04

FREQ_RANKS = 64
GRP_RANKS = 4
ROWS = NT // FREQ_RANKS
CHUNKS = 4
WIDTH = 256
SHARE = CHUNKS * WIDTH
JOINT = 4
TILES = NF // JOINT
UNROLL = 16
STEPS = TILES // UNROLL
MESH = pl.DeviceIdType.MESH


def transform_table():
    row_index = np.arange(2 * NF, dtype=np.int32)
    samples = np.arange(NT, dtype=np.int32)
    frequency = row_index // 8 * JOINT + row_index % JOINT
    parity = row_index // JOINT % 2
    turn_count = frequency[:, None] * samples[None, :] % NT
    angle_table = np.float32(2.0 * math.pi / NT) * turn_count.astype(np.float32)
    values = np.where(parity[:, None] == 0, np.cos(angle_table), -np.sin(angle_table))
    return (values / np.float32(math.sqrt(NT))).astype(jnp.bfloat16)


def kernel(
    source_hbm, table_hbm, position_hbm, blade_hbm, observers_hbm, index_hbm, out_ref,
    source, table, position, blade, observers, index, near, received, state, green_a, green_b, green_c, weighted, total,
    partial, gathered, share_out, share_in,
    load_sem, table_sem, small_sem, send_sem, recv_sem, sum_send, sum_recv, share_send, share_recv,
    x_sem, y_sem, group_sem,
):
    me = lax.axis_index("freq")
    group = lax.axis_index("grp")
    core, x, y, z = lax.rem(me, 2), lax.rem(lax.div(me, 2), 4), lax.rem(lax.div(me, 8), 4), lax.div(me, 32)
    xs = [2 * lax.rem(x + d, 4) for d in range(4)]
    ys = [8 * lax.rem(y + d, 4) for d in range(4)]
    zs = [32 * lax.rem(z + d // 2, 2) + lax.rem(core + d % 2, 2) for d in range(4)]
    along_x = [xs[d] + ys[0] + zs[0] for d in range(1, 4)]
    along_y = [xs[0] + ys[d] + zs[0] for d in range(1, 4)]
    along_z = [xs[0] + ys[0] + zs[d] for d in range(1, 4)]

    def signal(semaphore, device):
        pl.semaphore_signal(semaphore, inc=1, device_id={"freq": device}, device_id_type=MESH)

    def signal_groups(semaphore):
        for side in (1, GRP_RANKS - 1):
            other = lax.rem(group + side, GRP_RANKS)
            pl.semaphore_signal(semaphore, inc=1, device_id={"grp": other}, device_id_type=MESH)

    barrier = pltpu.get_barrier_semaphore()
    for device in along_x + along_y + along_z:
        signal(barrier, device)
    signal_groups(barrier)
    load = pltpu.make_async_copy(source_hbm, source, load_sem)
    load.start()
    share = pl.ds(pl.multiple_of(me * SHARE, SHARE), SHARE)
    small = [
        pltpu.make_async_copy(observers_hbm, observers, small_sem.at[0]),
        pltpu.make_async_copy(index_hbm, index, small_sem.at[1]),
        pltpu.make_async_copy(position_hbm.at[:, share], position, small_sem.at[2]),
        pltpu.make_async_copy(blade_hbm.at[pl.ds(pl.multiple_of(me * 8, 8), 8), :], blade, small_sem.at[3]),
    ]
    for copy in small:
        copy.start()
    table_load = pltpu.make_async_copy(table_hbm, table, table_sem)
    table_load.start()

    own_rows = pl.ds(pl.multiple_of(me * ROWS, ROWS), ROWS)

    def columns(device, chunk):
        return pl.ds(pl.multiple_of(device * SHARE + chunk * WIDTH, WIDTH), WIDTH)

    def send(device, chunk):
        pltpu.make_async_remote_copy(
            src_ref=source.at[:, columns(device, chunk)],
            dst_ref=received.at[chunk, own_rows, :],
            send_sem=send_sem.at[chunk],
            recv_sem=recv_sem.at[chunk],
            device_id={"freq": device},
            device_id_type=MESH,
        ).start()

    def seed(chunk):
        for half in range(WIDTH // 128):
            squares = None
            for axis in range(3):
                row = position[axis : axis + 1, pl.ds(chunk * WIDTH + half * 128, 128)]
                column = jnp.broadcast_to(row, (128, 128)).T
                offset = near[axis : axis + 1, :] - column
                squares = offset * offset if squares is None else squares + offset * offset
            inverse = lax.rsqrt(squares)
            distance = squares * inverse
            amplitude = (0.25 / math.pi) * inverse
            angle = wave_step * distance
            w = angle * angle
            cos1 = 1.0 + w * (-1 / 2 + w * (1 / 24 + w * (-1 / 720 + w * (1 / 40320 - w * (1 / 3628800)))))
            sin1 = angle * (1.0 + w * (-1 / 6 + w * (1 / 120 + w * (-1 / 5040 + w * (1 / 362880)))))
            cos2 = cos1 * cos1 - sin1 * sin1
            sin2 = 2.0 * sin1 * cos1
            cos3 = cos2 * cos1 - sin2 * sin1
            sin3 = sin2 * cos1 + cos2 * sin1
            cos4 = cos2 * cos2 - sin2 * sin2
            sin4 = 2.0 * sin2 * cos2
            lane = lax.broadcasted_iota(jnp.int32, (128, 128), 1) // NOBS
            cos_j = jnp.where(lane == 0, 1.0, jnp.where(lane == 1, cos1, jnp.where(lane == 2, cos2, cos3)))
            sin_j = jnp.where(lane == 0, 0.0, jnp.where(lane == 1, sin1, jnp.where(lane == 2, sin2, sin3)))
            rows = pl.ds(half * 128, 128)
            state[0, rows, :] = 2.0 * cos4
            state[1, rows, :] = amplitude * (cos_j * cos4 + sin_j * sin4)
            state[2, rows, :] = amplitude * cos_j
            state[3, rows, :] = -amplitude * (sin_j * cos4 - cos_j * sin4)
            state[4, rows, :] = -amplitude * sin_j

    load.wait()
    pl.semaphore_wait(barrier, 11)
    for device in along_x:
        signal(x_sem, device)
    signal_groups(group_sem)
    for d in range(3):
        for device in (along_x[d], along_y[d], along_z[d]):
            send(device, 0)
    for chunk in range(CHUNKS):
        pltpu.make_async_copy(
            source.at[:, columns(me, chunk)],
            received.at[chunk, own_rows, :],
            recv_sem.at[chunk],
        ).start()
    pl.semaphore_wait(x_sem, 3)
    for device in along_y:
        signal(y_sem, device)
    for d in range(1, 4):
        for e in range(1, 4):
            send(xs[(d + e) % 3 + 1] + ys[e] + zs[0], 0)
            send(xs[(d + e) % 3 + 1] + ys[0] + zs[e], 0)
    for copy in small:
        copy.wait()

    places = lax.broadcasted_iota(jnp.int32, (3, 2048), 1)
    lanes = lax.broadcasted_iota(jnp.int32, (3, 128), 1)
    whole = observers[...]
    chosen = jnp.zeros((3, 128), jnp.float32)
    for i in range(NOBS):
        picked = jnp.sum(jnp.where(places == index[i], whole, 0.0), axis=1, keepdims=True)
        chosen = jnp.where(lanes % NOBS == i, picked, chosen)
    near[...] = chosen

    pl.semaphore_wait(y_sem, 3)
    for d in range(4):
        for e in range(9):
            send(xs[(d + e) % 4] + ys[e // 3 + 1] + zs[e % 3 + 1], 0)
    seed(0)

    def send_some(step, chunk):
        turned = [2 * lax.rem(x + step + d, 4) for d in range(4)]
        half = lax.div(step, 4)
        lines = [8 * lax.rem(y + 2 * half + d, 4) for d in range(2)]
        for t in range(8):
            device = turned[t % 4] + lines[t // 4] + zs[(t + t // 4) % 4]
            if t == 0:
                pl.when(step > 0)(lambda: send(device, chunk))
            else:
                send(device, chunk)

    greens = (green_a, green_b, green_c, green_a)

    def grow(green, step, block):
        rows = pl.ds(block * 16, 16)
        twice = state[0, rows, :]
        re_old, re_new = state[1, rows, :], state[2, rows, :]
        im_old, im_new = state[3, rows, :], state[4, rows, :]
        for u in range(UNROLL):
            tile = step * UNROLL + u
            green[tile, rows, 0:128] = re_new.astype(jnp.bfloat16)
            green[tile, rows, 128:256] = im_new.astype(jnp.bfloat16)
            re_old, re_new = re_new, twice * re_new - re_old
            im_old, im_new = im_new, twice * im_new - im_old
        state[1, rows, :] = re_old
        state[2, rows, :] = re_new
        state[3, rows, :] = im_old
        state[4, rows, :] = im_new

    def grow_all(chunk, sent):
        def part(step, carry):
            if sent is not None:
                send_some(step, sent)
            for block in range(WIDTH // 16):
                grow(greens[chunk], step, block)
            return carry

        lax.fori_loop(0, STEPS, part, 0)

    grow_all(0, 1)
    seed(1)
    grow_all(1, None)
    seed(2)
    grow_all(2, 2)
    table_load.wait()

    sublane = lax.broadcasted_iota(jnp.int32, (8, 128), 0)
    lane_joint = lax.broadcasted_iota(jnp.int32, (8, 128), 1) // NOBS
    keep_a = (sublane == lane_joint).astype(jnp.float32)
    keep_c = (sublane == lane_joint + JOINT).astype(jnp.float32)

    def transform(chunk):
        blades = jnp.concatenate([blade[2 * chunk : 2 * chunk + 1, :], blade[2 * chunk + 1 : 2 * chunk + 2, :]], axis=1)
        masks = [(blades == b).astype(jnp.float32).reshape(1, 1, WIDTH) for b in range(NCOMP)]

        def part(i, carry):
            spectrum = jnp.dot(
                table[pl.ds(pl.multiple_of(i * 256, 256), 256), :],
                received[chunk],
                preferred_element_type=jnp.float32,
            ).reshape(32, 8, WIDTH)
            for pair in range(NCOMP // 2):
                both = jnp.concatenate([spectrum * masks[2 * pair], spectrum * masks[2 * pair + 1]], axis=1)
                weighted[pl.ds(i * 32, 32), pl.ds(16 * pair, 16), :] = both.astype(jnp.bfloat16)
            return carry

        lax.fori_loop(0, 4, part, 0)

    def pressure(value):
        sums = []
        for blade in range(NCOMP):
            re_side = value[8 * blade : 8 * blade + 8, 0:128]
            im_side = value[8 * blade : 8 * blade + 8, 128:256]
            sums.append(jnp.sum(re_side * keep_a - im_side * keep_c, axis=0, keepdims=True))
            sums.append(jnp.sum(im_side * keep_a + re_side * keep_c, axis=0, keepdims=True))
        return jnp.concatenate(sums, axis=0)

    def far_first(step):
        t = lax.rem(step, 4)
        line = lax.rem(y + 2 - t + 3 * lax.div(t, 2) + 2 * lax.div(t, 3), 4)
        return lax.rem(z + 1 - lax.div(step, 4), 2) * 4 + line

    def send_sums(step):
        for u in range(UNROLL // 2):
            device = far_first(step) * (UNROLL // 2) + u

            @pl.when(device != me)
            def _():
                pltpu.make_async_remote_copy(
                    src_ref=partial.at[device],
                    dst_ref=gathered.at[me],
                    send_sem=sum_send,
                    recv_sem=sum_recv,
                    device_id={"freq": device},
                    device_id_type=MESH,
                ).start()

    for chunk in range(CHUNKS):
        pltpu.make_async_copy(received.at[chunk], received.at[chunk], recv_sem.at[chunk]).wait()
        transform(chunk)
        last = chunk == CHUNKS - 1
        if chunk == 1:
            seed(3)

        def contract(step, carry):
            if chunk == 0:
                send_some(step, 3)
            if last:

                @pl.when(step > 0)
                def _():
                    send_sums(step - 1)

            rows = []
            place = far_first(step) if last else step
            for u in range(UNROLL):
                tile = place * UNROLL + u
                product = jnp.dot(weighted[tile], greens[chunk][tile], preferred_element_type=jnp.float32)
                if chunk > 0:
                    product = total[tile] + product
                if last:
                    rows.append(pressure(product))
                else:
                    total[tile] = product
                if chunk == 1:
                    grow(greens[3], step, u)
            if last:
                for u in range(UNROLL // 2):
                    both = jnp.concatenate([rows[2 * u], rows[2 * u + 1]], axis=0)
                    partial[place * (UNROLL // 2) + u] = both.astype(jnp.bfloat16)
            return carry

        lax.fori_loop(0, STEPS, contract, 0)

    own = pltpu.make_async_copy(partial.at[me], gathered.at[me], sum_recv)
    own.start()
    send_sums(STEPS - 1)
    pltpu.make_async_copy(gathered, gathered, sum_recv).wait()

    def add(i, carry):
        return carry + jnp.sum(gathered[pl.ds(i * 8, 8)].astype(jnp.float32), axis=0)

    summed = lax.fori_loop(0, FREQ_RANKS // 8, add, jnp.zeros((16, 128), jnp.float32))
    for blade in range(NCOMP):
        share_out[blade, 0:2, :] = summed[2 * blade : 2 * blade + 2, :]
        share_out[blade, 2:4, :] = summed[8 + 2 * blade : 8 + 2 * blade + 2, :]
        share_out[blade, 4:8, :] = jnp.zeros((4, 128), jnp.float32)
    pl.semaphore_wait(group_sem, 2)
    for i in range(1, GRP_RANKS):
        other = lax.rem(group + i, GRP_RANKS)
        pltpu.make_async_remote_copy(
            src_ref=share_out.at[other],
            dst_ref=share_in.at[group],
            send_sem=share_send,
            recv_sem=share_recv,
            device_id={"grp": other},
            device_id_type=MESH,
        ).start()
    pltpu.make_async_copy(share_out.at[group], share_in.at[group], share_recv).start()
    pltpu.make_async_copy(share_in, share_in, share_recv).wait()
    result = share_in[0] + share_in[1] + share_in[2] + share_in[3]
    for m in range(2):
        for j in range(JOINT):
            for part in range(2):
                out_ref[JOINT * m + j, 0, part : part + 1, :] = result[
                    2 * m + part : 2 * m + part + 1, NOBS * j : NOBS * (j + 1)
                ]

    for chunk in range(CHUNKS):
        sent = received.at[chunk, pl.ds(0, ROWS * (FREQ_RANKS - 1)), :]
        pltpu.make_async_copy(sent, sent, send_sem.at[chunk]).wait()
    sent = gathered.at[pl.ds(0, FREQ_RANKS - 1)]
    pltpu.make_async_copy(sent, sent, sum_send).wait()
    sent = share_in.at[pl.ds(0, GRP_RANKS - 1)]
    pltpu.make_async_copy(sent, sent, share_send).wait()


def body(sources, panel_pos, panel_blade, observer_table, observer_index):
    bf16, f32 = jnp.bfloat16, jnp.float32
    dma, regular = pltpu.SemaphoreType.DMA, pltpu.SemaphoreType.REGULAR
    out = pl.pallas_call(
        kernel,
        out_shape=jax.ShapeDtypeStruct((8, 1, 2, NOBS), f32),
        in_specs=[pl.BlockSpec(memory_space=pl.ANY)] * 6,
        out_specs=pl.BlockSpec(memory_space=pltpu.VMEM),
        scratch_shapes=[
            pltpu.VMEM((ROWS, FREQ_RANKS * SHARE), bf16),
            pltpu.VMEM((2 * NF, NT), bf16),
            pltpu.VMEM((3, SHARE), f32),
            pltpu.VMEM((8, 128), jnp.int32),
            pltpu.VMEM((3, 2048), f32),
            pltpu.SMEM((NOBS,), jnp.int32),
            pltpu.VMEM((3, 128), f32),
            pltpu.VMEM((CHUNKS, NT, WIDTH), bf16),
            pltpu.VMEM((5, WIDTH, 128), f32),
            pltpu.VMEM((TILES, WIDTH, 256), bf16),
            pltpu.VMEM((TILES, WIDTH, 256), bf16),
            pltpu.VMEM((TILES, WIDTH, 256), bf16),
            pltpu.VMEM((TILES, 32, WIDTH), bf16),
            pltpu.VMEM((TILES, 32, 256), f32),
            pltpu.VMEM((FREQ_RANKS, 16, 128), bf16),
            pltpu.VMEM((FREQ_RANKS, 16, 128), bf16),
            pltpu.VMEM((NCOMP, 8, 128), f32),
            pltpu.VMEM((GRP_RANKS, 8, 128), f32),
            dma, dma, dma((4,)), dma((CHUNKS,)), dma((CHUNKS,)), dma, dma, dma, dma,
            regular, regular, regular,
        ],
        compiler_params=pltpu.CompilerParams(
            collective_id=0, has_side_effects=True, vmem_limit_bytes=67043328
        ),
    )(sources, jnp.asarray(transform_table()), panel_pos, panel_blade.reshape(-1, 128), observer_table, observer_index)
    return out


def solution(mesh):
    in_specs = (P("freq", "grp"), P(None, "grp"), P("grp"), P(), P())
    out_specs = P("freq", "grp", None, None)
    return jax.shard_map(body, mesh=mesh, in_specs=in_specs, out_specs=out_specs, check_vma=False)
```

```python
import math

import jax
import jax.numpy as jnp
import numpy as np
from jax import lax
from jax.experimental import pallas as pl
from jax.experimental.pallas import tpu as pltpu
from jax.sharding import PartitionSpec as P

NT = 1024
NF = 512
NCOMP = 4
NOBS = 32

wave_step = 0.04

FREQ_RANKS = 64
GRP_RANKS = 4
ROWS = NT // FREQ_RANKS
CHUNKS = 4
WIDTH = 256
SHARE = CHUNKS * WIDTH
JOINT = 4
TILES = NF // JOINT
UNROLL = 16
STEPS = TILES // UNROLL
MESH = pl.DeviceIdType.MESH


def transform_table():
    row_index = np.arange(2 * NF, dtype=np.int32)
    samples = np.arange(NT, dtype=np.int32)
    frequency = row_index // 8 * JOINT + row_index % JOINT
    parity = row_index // JOINT % 2
    turn_count = frequency[:, None] * samples[None, :] % NT
    angle_table = np.float32(2.0 * math.pi / NT) * turn_count.astype(np.float32)
    values = np.where(parity[:, None] == 0, np.cos(angle_table), -np.sin(angle_table))
    return (values / np.float32(math.sqrt(NT))).astype(jnp.bfloat16)


def kernel(
    source_hbm, table_hbm, position_hbm, blade_hbm, observers_hbm, index_hbm, out_ref,
    source, table, position, blade, observers, index, near, received, state, green_a, green_b, green_c, weighted, total,
    partial, gathered, share_out, share_in,
    load_sem, table_sem, small_sem, send_sem, recv_sem, sum_send, sum_recv, share_send, share_recv,
    group_sem,
):
    me = lax.axis_index("freq")
    group = lax.axis_index("grp")
    core, x, y, z = lax.rem(me, 2), lax.rem(lax.div(me, 2), 4), lax.rem(lax.div(me, 8), 4), lax.div(me, 32)
    xs = [2 * lax.rem(x + d, 4) for d in range(4)]
    ys = [8 * lax.rem(y + d, 4) for d in range(4)]
    zs = [32 * lax.rem(z + d // 2, 2) + lax.rem(core + d % 2, 2) for d in range(4)]
    def signal(semaphore, device):
        pl.semaphore_signal(semaphore, inc=1, device_id={"freq": device}, device_id_type=MESH)

    def signal_groups(semaphore):
        for side in (1, GRP_RANKS - 1):
            other = lax.rem(group + side, GRP_RANKS)
            pl.semaphore_signal(semaphore, inc=1, device_id={"grp": other}, device_id_type=MESH)

    load = pltpu.make_async_copy(source_hbm, source, load_sem)
    load.start()
    barrier = pltpu.get_barrier_semaphore()
    for t in range(63, 0, -1):
        signal(barrier, xs[t % 4] + ys[t // 4 % 4] + zs[t // 16])
    signal_groups(barrier)
    share = pl.ds(pl.multiple_of(me * SHARE, SHARE), SHARE)
    small = [
        pltpu.make_async_copy(observers_hbm, observers, small_sem.at[0]),
        pltpu.make_async_copy(index_hbm, index, small_sem.at[1]),
        pltpu.make_async_copy(position_hbm.at[:, share], position, small_sem.at[2]),
        pltpu.make_async_copy(blade_hbm.at[pl.ds(pl.multiple_of(me * 8, 8), 8), :], blade, small_sem.at[3]),
    ]
    for copy in small:
        copy.start()
    table_load = pltpu.make_async_copy(table_hbm, table, table_sem)
    table_load.start()

    own_rows = pl.ds(pl.multiple_of(me * ROWS, ROWS), ROWS)

    def columns(device, chunk):
        return pl.ds(pl.multiple_of(device * SHARE + chunk * WIDTH, WIDTH), WIDTH)

    def send(device, chunk):
        pltpu.make_async_remote_copy(
            src_ref=source.at[:, columns(device, chunk)],
            dst_ref=received.at[chunk, own_rows, :],
            send_sem=send_sem.at[chunk],
            recv_sem=recv_sem.at[chunk],
            device_id={"freq": device},
            device_id_type=MESH,
        ).start()

    def seed(chunk):
        for half in range(WIDTH // 128):
            squares = None
            for axis in range(3):
                row = position[axis : axis + 1, pl.ds(chunk * WIDTH + half * 128, 128)]
                column = jnp.broadcast_to(row, (128, 128)).T
                offset = near[axis : axis + 1, :] - column
                squares = offset * offset if squares is None else squares + offset * offset
            inverse = lax.rsqrt(squares)
            distance = squares * inverse
            amplitude = (0.25 / math.pi) * inverse
            angle = wave_step * distance
            w = angle * angle
            cos1 = 1.0 + w * (-1 / 2 + w * (1 / 24 + w * (-1 / 720 + w * (1 / 40320 - w * (1 / 3628800)))))
            sin1 = angle * (1.0 + w * (-1 / 6 + w * (1 / 120 + w * (-1 / 5040 + w * (1 / 362880)))))
            cos2 = cos1 * cos1 - sin1 * sin1
            sin2 = 2.0 * sin1 * cos1
            cos3 = cos2 * cos1 - sin2 * sin1
            sin3 = sin2 * cos1 + cos2 * sin1
            cos4 = cos2 * cos2 - sin2 * sin2
            sin4 = 2.0 * sin2 * cos2
            lane = lax.broadcasted_iota(jnp.int32, (128, 128), 1) // NOBS
            cos_j = jnp.where(lane == 0, 1.0, jnp.where(lane == 1, cos1, jnp.where(lane == 2, cos2, cos3)))
            sin_j = jnp.where(lane == 0, 0.0, jnp.where(lane == 1, sin1, jnp.where(lane == 2, sin2, sin3)))
            rows = pl.ds(half * 128, 128)
            state[0, rows, :] = 2.0 * cos4
            state[1, rows, :] = amplitude * (cos_j * cos4 + sin_j * sin4)
            state[2, rows, :] = amplitude * cos_j
            state[3, rows, :] = -amplitude * (sin_j * cos4 - cos_j * sin4)
            state[4, rows, :] = -amplitude * sin_j

    for copy in small:
        copy.wait()

    places = lax.broadcasted_iota(jnp.int32, (3, 2048), 1)
    lanes = lax.broadcasted_iota(jnp.int32, (3, 128), 1)
    whole = observers[...]
    chosen = jnp.zeros((3, 128), jnp.float32)
    for i in range(NOBS):
        picked = jnp.sum(jnp.where(places == index[i], whole, 0.0), axis=1, keepdims=True)
        chosen = jnp.where(lanes % NOBS == i, picked, chosen)
    near[...] = chosen

    seed(0)
    load.wait()
    pl.semaphore_wait(barrier, 65)
    signal_groups(group_sem)
    for chunk in range(CHUNKS):
        pltpu.make_async_copy(
            source.at[:, columns(me, chunk)],
            received.at[chunk, own_rows, :],
            recv_sem.at[chunk],
        ).start()
    def send_some(step, chunk):
        turned = [2 * lax.rem(x + step + d, 4) for d in range(4)]
        half = lax.div(step, 4)
        lines = [8 * lax.rem(y + 2 * half + d, 4) for d in range(2)]
        for t in range(8):
            device = turned[t % 4] + lines[t // 4] + zs[(t + t // 4) % 4]
            if t == 0:
                pl.when(step > 0)(lambda: send(device, chunk))
            else:
                send(device, chunk)

    greens = (green_a, green_b, green_c, green_a)

    def grow(green, step, block):
        rows = pl.ds(block * 16, 16)
        twice = state[0, rows, :]
        re_old, re_new = state[1, rows, :], state[2, rows, :]
        im_old, im_new = state[3, rows, :], state[4, rows, :]
        for u in range(UNROLL):
            tile = step * UNROLL + u
            green[tile, rows, 0:128] = re_new.astype(jnp.bfloat16)
            green[tile, rows, 128:256] = im_new.astype(jnp.bfloat16)
            re_old, re_new = re_new, twice * re_new - re_old
            im_old, im_new = im_new, twice * im_new - im_old
        state[1, rows, :] = re_old
        state[2, rows, :] = re_new
        state[3, rows, :] = im_old
        state[4, rows, :] = im_new

    def grow_all(chunk, sent):
        def part(step, carry):
            if sent is not None:
                send_some(step, sent)
            for block in range(WIDTH // 16):
                grow(greens[chunk], step, block)
            return carry

        lax.fori_loop(0, STEPS, part, 0)

    lax.fori_loop(0, 8, lambda step, c: (send_some(step, 0), c)[1], 0)
    grow_all(0, 1)
    seed(1)
    grow_all(1, 2)
    seed(2)
    grow_all(2, 3)
    table_load.wait()

    sublane = lax.broadcasted_iota(jnp.int32, (8, 128), 0)
    lane_joint = lax.broadcasted_iota(jnp.int32, (8, 128), 1) // NOBS
    keep_a = (sublane == lane_joint).astype(jnp.float32)
    keep_c = (sublane == lane_joint + JOINT).astype(jnp.float32)

    def transform(chunk):
        blades = jnp.concatenate([blade[2 * chunk : 2 * chunk + 1, :], blade[2 * chunk + 1 : 2 * chunk + 2, :]], axis=1)
        masks = [(blades == b).astype(jnp.float32).reshape(1, 1, WIDTH) for b in range(NCOMP)]

        def part(i, carry):
            spectrum = jnp.dot(
                table[pl.ds(pl.multiple_of(i * 256, 256), 256), :],
                received[chunk],
                preferred_element_type=jnp.float32,
            ).reshape(32, 8, WIDTH)
            for pair in range(NCOMP // 2):
                both = jnp.concatenate([spectrum * masks[2 * pair], spectrum * masks[2 * pair + 1]], axis=1)
                weighted[pl.ds(i * 32, 32), pl.ds(16 * pair, 16), :] = both.astype(jnp.bfloat16)
            return carry

        lax.fori_loop(0, 4, part, 0)

    def pressure(value):
        sums = []
        for blade in range(NCOMP):
            re_side = value[8 * blade : 8 * blade + 8, 0:128]
            im_side = value[8 * blade : 8 * blade + 8, 128:256]
            sums.append(jnp.sum(re_side * keep_a - im_side * keep_c, axis=0, keepdims=True))
            sums.append(jnp.sum(im_side * keep_a + re_side * keep_c, axis=0, keepdims=True))
        return jnp.concatenate(sums, axis=0)

    def far_first(step):
        t = lax.rem(step, 4)
        line = lax.rem(y + 2 - t + 3 * lax.div(t, 2) + 2 * lax.div(t, 3), 4)
        return lax.rem(z + 1 - lax.div(step, 4), 2) * 4 + line

    def send_sums(step):
        for u in range(UNROLL // 2):
            device = far_first(step) * (UNROLL // 2) + u

            @pl.when(device != me)
            def _():
                pltpu.make_async_remote_copy(
                    src_ref=partial.at[device],
                    dst_ref=gathered.at[me],
                    send_sem=sum_send,
                    recv_sem=sum_recv,
                    device_id={"freq": device},
                    device_id_type=MESH,
                ).start()

    for chunk in range(CHUNKS):
        pltpu.make_async_copy(received.at[chunk], received.at[chunk], recv_sem.at[chunk]).wait()
        transform(chunk)
        last = chunk == CHUNKS - 1
        if chunk == 1:
            seed(3)

        def contract(step, carry):
            if last:

                @pl.when(step > 0)
                def _():
                    send_sums(step - 1)

            rows = []
            place = far_first(step) if last else step
            for u in range(UNROLL):
                tile = place * UNROLL + u
                product = jnp.dot(weighted[tile], greens[chunk][tile], preferred_element_type=jnp.float32)
                if chunk > 0:
                    product = total[tile] + product
                if last:
                    rows.append(pressure(product))
                else:
                    total[tile] = product
                if chunk == 1:
                    grow(greens[3], step, u)
            if last:
                for u in range(UNROLL // 2):
                    both = jnp.concatenate([rows[2 * u], rows[2 * u + 1]], axis=0)
                    partial[place * (UNROLL // 2) + u] = both.astype(jnp.bfloat16)
            return carry

        lax.fori_loop(0, STEPS, contract, 0)

    own = pltpu.make_async_copy(partial.at[me], gathered.at[me], sum_recv)
    own.start()
    send_sums(STEPS - 1)
    pltpu.make_async_copy(gathered, gathered, sum_recv).wait()

    def add(i, carry):
        return carry + jnp.sum(gathered[pl.ds(i * 8, 8)].astype(jnp.float32), axis=0)

    summed = lax.fori_loop(0, FREQ_RANKS // 8, add, jnp.zeros((16, 128), jnp.float32))
    for blade in range(NCOMP):
        share_out[blade, 0:2, :] = summed[2 * blade : 2 * blade + 2, :]
        share_out[blade, 2:4, :] = summed[8 + 2 * blade : 8 + 2 * blade + 2, :]
        share_out[blade, 4:8, :] = jnp.zeros((4, 128), jnp.float32)
    pl.semaphore_wait(group_sem, 2)
    for i in range(1, GRP_RANKS):
        other = lax.rem(group + i, GRP_RANKS)
        pltpu.make_async_remote_copy(
            src_ref=share_out.at[other],
            dst_ref=share_in.at[group],
            send_sem=share_send,
            recv_sem=share_recv,
            device_id={"grp": other},
            device_id_type=MESH,
        ).start()
    pltpu.make_async_copy(share_out.at[group], share_in.at[group], share_recv).start()
    pltpu.make_async_copy(share_in, share_in, share_recv).wait()
    result = share_in[0] + share_in[1] + share_in[2] + share_in[3]
    for m in range(2):
        for j in range(JOINT):
            for part in range(2):
                out_ref[JOINT * m + j, 0, part : part + 1, :] = result[
                    2 * m + part : 2 * m + part + 1, NOBS * j : NOBS * (j + 1)
                ]

    for chunk in range(CHUNKS):
        sent = received.at[chunk, pl.ds(0, ROWS * (FREQ_RANKS - 1)), :]
        pltpu.make_async_copy(sent, sent, send_sem.at[chunk]).wait()
    sent = gathered.at[pl.ds(0, FREQ_RANKS - 1)]
    pltpu.make_async_copy(sent, sent, sum_send).wait()
    sent = share_in.at[pl.ds(0, GRP_RANKS - 1)]
    pltpu.make_async_copy(sent, sent, share_send).wait()


def body(sources, panel_pos, panel_blade, observer_table, observer_index):
    bf16, f32 = jnp.bfloat16, jnp.float32
    dma, regular = pltpu.SemaphoreType.DMA, pltpu.SemaphoreType.REGULAR
    out = pl.pallas_call(
        kernel,
        out_shape=jax.ShapeDtypeStruct((8, 1, 2, NOBS), f32),
        in_specs=[pl.BlockSpec(memory_space=pl.ANY)] * 6,
        out_specs=pl.BlockSpec(memory_space=pltpu.VMEM),
        scratch_shapes=[
            pltpu.VMEM((ROWS, FREQ_RANKS * SHARE), bf16),
            pltpu.VMEM((2 * NF, NT), bf16),
            pltpu.VMEM((3, SHARE), f32),
            pltpu.VMEM((8, 128), jnp.int32),
            pltpu.VMEM((3, 2048), f32),
            pltpu.SMEM((NOBS,), jnp.int32),
            pltpu.VMEM((3, 128), f32),
            pltpu.VMEM((CHUNKS, NT, WIDTH), bf16),
            pltpu.VMEM((5, WIDTH, 128), f32),
            pltpu.VMEM((TILES, WIDTH, 256), bf16),
            pltpu.VMEM((TILES, WIDTH, 256), bf16),
            pltpu.VMEM((TILES, WIDTH, 256), bf16),
            pltpu.VMEM((TILES, 32, WIDTH), bf16),
            pltpu.VMEM((TILES, 32, 256), f32),
            pltpu.VMEM((FREQ_RANKS, 16, 128), bf16),
            pltpu.VMEM((FREQ_RANKS, 16, 128), bf16),
            pltpu.VMEM((NCOMP, 8, 128), f32),
            pltpu.VMEM((GRP_RANKS, 8, 128), f32),
            dma, dma, dma((4,)), dma((CHUNKS,)), dma((CHUNKS,)), dma, dma, dma, dma,
            regular,
        ],
        compiler_params=pltpu.CompilerParams(
            collective_id=0, has_side_effects=True, vmem_limit_bytes=67043328
        ),
    )(sources, jnp.asarray(transform_table()), panel_pos, panel_blade.reshape(-1, 128), observer_table, observer_index)
    return out


def solution(mesh):
    in_specs = (P("freq", "grp"), P(None, "grp"), P("grp"), P(), P())
    out_specs = P("freq", "grp", None, None)
    return jax.shard_map(body, mesh=mesh, in_specs=in_specs, out_specs=out_specs, check_vma=False)
```
